32 devices in a mesh: strip: 8 (over z, x), col: 4 (over y, core).
Axes of the slice: x: 2, y: 2, z: 4, core: 2. Of those that a mesh axis runs over, the one named last changes fastest.
Arguments:
- residuals: float32 [16, 64, 2560], P('strip'), may hold values from -6 to 6
- corr_rows: float32 [64], replicated, may hold values from 0.5 to 2
- corr_cols: float32 [2560], replicated, may hold values from 0.5 to 2
- row_anchor: int32 [16], replicated, may hold values from 0 to 64
- col_anchor: int32 [16], replicated, may hold values from 0 to 7680
- valid_first: int32 [16], replicated, may hold values from 0 to 15
- valid_end: int32 [16], replicated, may hold values from 49 to 64
- facet_of_slot: int32 [16], replicated, may hold values from 0 to 15, each once
Outputs:
- stitched: float32 [128, 10240], P('strip', 'col')
- column_power: float32 [10240], P('col')
The draws below stay inside these ranges and needn't reach their ends.
Inputs may be any that keep to these rules, and one draw needn't show every extreme that they name: facet_of_slot names each of the 16 facets exactly once.
All inputs are finite; a program needn't handle non-finite values.
Results may differ from the reference program's by a relative error of at most 0.0003.
Values sent between devices are 32-bit elements; how exact they have to be, the bound alone decides.
A program may use at most 64 MiB of HBM per device.

```python
import math
import jax
import jax.numpy as jnp
from jax import lax

FW = 2560
FH = 64
FACETS = 16
MH = 128
MW = 10240


def with_ends(array, stream_key, low, largest):
    place = [jax.random.randint(jax.random.fold_in(stream_key, axis), (), 0, length) for axis, length in enumerate(array.shape)]
    longest = array.shape.index(max(array.shape))
    neighbour = place[:longest] + [(place[longest] + 1) % array.shape[longest]] + place[longest + 1:]
    return array.at[tuple(place)].set(low).at[tuple(neighbour)].set(largest)


def level_of(rng, shape, shards, smallest, high):
    loudness, own = 1.0, jax.random.fold_in(rng, 6)
    for dim, parts in shards:
        steps = jnp.exp(jax.random.uniform(jax.random.fold_in(own, dim), (parts,), jnp.float32, smallest / len(shards), high / len(shards)))
        loudness = loudness * jnp.repeat(steps, shape[dim] // parts).reshape([-1 if axis == dim else 1 for axis in range(len(shape))])
    return loudness


def scatter_about(rng, extent, deviation, most, split=(), dtype=jnp.bfloat16):
    entries = jax.random.normal(rng, extent, jnp.float32) * deviation
    if len(split) > 0:
        entries = level_of(rng, extent, split, -0.22, 0.18) * entries
    return jnp.clip(entries, min=-most, max=most).astype(dtype)


def setup_inputs(seed: int = 0) -> dict:
    keys = jax.random.split(jax.random.key(seed), 9)
    residuals = scatter_about(keys[0], (FACETS, FH, FW), 1.0, 6.0, ((0, 8),), jnp.float32)
    corr_rows = jnp.clip(jnp.exp(jax.random.uniform(keys[1], (FH,), jnp.float32, math.log(0.5), math.log(2.0))), 0.5, 2.0)
    corr_cols = jnp.clip(jnp.exp(jax.random.uniform(keys[2], (FW,), jnp.float32, math.log(0.5), math.log(2.0))), 0.5, 2.0)
    row_anchor = with_ends(jax.random.randint(keys[3], (FACETS,), 0, MH - FH + 1), jax.random.fold_in(keys[3], 1), 0, MH - FH).astype(jnp.int32)
    col_anchor = with_ends(jax.random.randint(keys[4], (FACETS,), 0, MW - FW + 1), jax.random.fold_in(keys[4], 1), 0, MW - FW).astype(jnp.int32)
    valid_first = with_ends(jax.random.randint(keys[5], (FACETS,), 0, FH // 4), jax.random.fold_in(keys[5], 1), 0, (FH // 4) - 1).astype(jnp.int32)
    valid_end = with_ends(jax.random.randint(keys[6], (FACETS,), 3 * FH // 4 + 1, FH + 1), jax.random.fold_in(keys[6], 1), 3 * FH // 4 + 1, FH).astype(jnp.int32)
    facet_of_slot = jax.random.permutation(keys[7], FACETS).astype(jnp.int32)
    return dict(residuals=residuals, corr_rows=corr_rows, corr_cols=corr_cols, row_anchor=row_anchor, col_anchor=col_anchor, valid_first=valid_first, valid_end=valid_end, facet_of_slot=facet_of_slot)


def tapers(count):
    position = (jnp.arange(count).astype(jnp.float32) + 0.5) / count
    return jnp.sin(jnp.pi * position) ** 2


def reference(residuals, corr_rows, corr_cols, row_anchor, col_anchor, valid_first, valid_end, facet_of_slot):
    facet_rows = residuals.shape[1]
    facet_cols = residuals.shape[2]
    row_index = jnp.arange(facet_rows).astype(jnp.int32)
    row_taper = tapers(facet_rows)
    col_taper = tapers(facet_cols)
    correction = corr_rows[:, None] * corr_cols[None, :]

    def accumulate(running, position):
        numerator, denominator = running
        facet_id = facet_of_slot[position]
        row_start = row_anchor[facet_id]
        col_start = col_anchor[facet_id]
        inside = (row_index >= valid_first[facet_id]) & (row_index < valid_end[facet_id])
        row_weight = jnp.where(inside, row_taper, 0.0)
        weight = row_weight[:, None] * col_taper[None, :]
        weighted = weight * correction * residuals[position]
        old_num = lax.dynamic_slice(numerator, (row_start, col_start), (facet_rows, facet_cols))
        numerator = lax.dynamic_update_slice(numerator, old_num + weighted, (row_start, col_start))
        old_den = lax.dynamic_slice(denominator, (row_start, col_start), (facet_rows, facet_cols))
        denominator = lax.dynamic_update_slice(denominator, old_den + weight, (row_start, col_start))
        return (numerator, denominator), None

    blank = jnp.zeros((MH, MW), jnp.float32)
    (numerator, denominator), _ = lax.scan(accumulate, (blank, blank), jnp.arange(FACETS).astype(jnp.int32))
    stitched = numerator / jnp.maximum(denominator, 0.5)
    column_power = jnp.mean(stitched * stitched, axis=0)
    return (stitched, column_power)
```

```python
import functools
import math

import jax
import jax.numpy as jnp
from jax import lax
from jax.experimental import pallas as pl
from jax.experimental.pallas import tpu as pltpu
from jax.sharding import PartitionSpec as P

MESH = pl.DeviceIdType.MESH
CHUNKS = 2


def taper(position, count):
    angle = (position.astype(jnp.float32) + (0.5 - count / 2)) * (math.pi / count)
    square = angle * angle
    value = jnp.full_like(square, 1.0 / math.factorial(12))
    for order in (10, 8, 6, 4, 2, 0):
        sign = -1.0 if order % 4 == 2 else 1.0
        value = value * square + sign / math.factorial(order)
    return value * value


def visit_order(count):
    return [sorted(range(count), key=lambda d: (-abs(d - z), d < z)) for z in range(count)]


def place_kernel(
    strips, lanes, fid_ref, ra_ref, ca_ref, vf_ref, ve_ref, rows_ref, cols_ref, res_ref,
    blocks_ref, placed,
):
    local, fh, fw = res_ref.shape
    height = fh // 4
    width = fw // CHUNKS
    strip = lax.axis_index("strip")
    group = lax.axis_index("col")

    eye = lax.broadcasted_iota(jnp.int32, (fh, fh), 0) == lax.broadcasted_iota(
        jnp.int32, (fh, fh), 1
    )
    corr_row = jnp.sum(jnp.where(eye, rows_ref[...], 0.0), axis=1, keepdims=True)
    y = lax.broadcasted_iota(jnp.int32, (fh, 1), 0)
    u = lax.broadcasted_iota(jnp.int32, (1, fw), 1)
    row_taper = taper(y, fh)
    col_scale = taper(u, fw) * cols_ref[...]
    blank = jnp.zeros((height, fw), jnp.float32)
    sub = lax.broadcasted_iota(jnp.int32, (8, 1), 0)
    anchors = []
    for p in range(local):
        f = fid_ref[strip * local + p]
        ra, ca = ra_ref[f], ca_ref[f]
        anchors.append(ra)
        inside = (y >= vf_ref[f]) & (y < ve_ref[f])
        row_scale = jnp.where(inside, row_taper, 0.0) * corr_row
        col_pos = u + (group * fw - ca)
        col_inside = (col_pos >= 0) & (col_pos < fw)
        shift = lax.rem(ca, fw)
        lift = lax.rem(ra, 8)
        placed[p, pl.ds(0, height), :] = blank
        placed[p, pl.ds(height + fh + 8, height), :] = blank
        held = jnp.zeros((8, fw), jnp.float32)
        for row in range(0, fh, 8):
            term = res_ref[p, pl.ds(row, 8), :] * col_scale * row_scale[row : row + 8]
            term = jnp.where(col_inside, pltpu.roll(term, shift, axis=1), 0.0)
            term = pltpu.roll(term, lift, axis=0)
            placed[p, pl.ds(height + row, 8), :] = jnp.where(sub < lift, held, term)
            held = term
        placed[p, pl.ds(height + fh, 8), :] = jnp.where(sub < lift, held, 0.0)

    def place(block, chunk):
        total = None
        for p in range(local):
            tile = block * (height // 8) - lax.div(anchors[p], 8)
            start = (jnp.clip(tile, -height // 8, fh // 8 + 1) + height // 8) * 8
            start = pl.multiple_of(start, 8)
            part = placed[p, pl.ds(start, height), pl.ds(chunk * width, width)]
            total = part if total is None else total + part
        return total

    for block in range(strips):
        for c in range(CHUNKS):
            blocks_ref[block // lanes, block % lanes, c] = place(block, c)


def kernel(
    strips, lanes, ra_ref, ca_ref, vf_ref, ve_ref, blocks_ref,
    out_ref, power_ref, den, xrecv, zsend, zrecv, psend, precv,
    xs_sem, xr_sem, zs_sem, zr_sem, ps_sem, pr_sem,
):
    facets = ra_ref.shape[0]
    height, fw = out_ref.shape
    fh = 4 * height
    levels = strips // lanes
    width = fw // CHUNKS
    strip = lax.axis_index("strip")
    group = lax.axis_index("col")
    z, x = lax.div(strip, lanes), lax.rem(strip, lanes)

    barrier = pltpu.get_barrier_semaphore()
    for k in range(1, strips):
        peer = lax.rem(strip + k, strips)
        pl.semaphore_signal(barrier, inc=1, device_id={"strip": peer}, device_id_type=MESH)

    order = visit_order(levels)

    def dest(t):
        d = jnp.int32(order[0][t])
        for place_z in range(1, levels):
            d = jnp.where(z == place_z, jnp.int32(order[place_z][t]), d)
        return d

    def x_copy(k, d, c):
        return pltpu.make_async_remote_copy(
            src_ref=blocks_ref.at[d, lax.rem(x + k, lanes), c],
            dst_ref=xrecv.at[k - 1, d, c],
            send_sem=xs_sem.at[k - 1, d, c],
            recv_sem=xr_sem.at[k - 1, d, c],
            device_id={"strip": z * lanes + lax.rem(x + k, lanes)},
            device_id_type=MESH,
        )

    def z_copy(way, d, c, target):
        return pltpu.make_async_remote_copy(
            src_ref=zsend.at[d, c],
            dst_ref=zrecv.at[way, d, c],
            send_sem=zs_sem.at[d, c],
            recv_sem=zr_sem.at[way, d, c],
            device_id={"strip": target * lanes + x},
            device_id_type=MESH,
        )

    def p_copy(k):
        return pltpu.make_async_remote_copy(
            src_ref=psend,
            dst_ref=precv.at[k - 1],
            send_sem=ps_sem.at[k - 1],
            recv_sem=pr_sem.at[k - 1],
            device_id={"strip": lax.rem(strip + k, strips)},
            device_id_type=MESH,
        )

    pl.semaphore_wait(barrier, strips - 1)
    for t in range(levels):
        d = dest(t)
        for c in range(CHUNKS):
            for k in range(1, lanes):
                x_copy(k, d, c).start()

    v = lax.broadcasted_iota(jnp.int32, (height, 1), 0) + strip * height
    u8 = lax.broadcasted_iota(jnp.int32, (8, fw), 1) + group * fw

    den[...] = jnp.zeros_like(den)

    def add_facet(f, carry):
        row_pos = v - ra_ref[f]
        row_inside = (row_pos >= vf_ref[f]) & (row_pos < ve_ref[f])
        row_part = jnp.where(row_inside, taper(row_pos, fh), 0.0)
        col_pos = u8 - ca_ref[f]
        col_inside = (col_pos >= 0) & (col_pos < fw)
        col_part = jnp.where(col_inside, taper(col_pos, fw), 0.0)
        for row in range(0, height, 8):
            den[pl.ds(row, 8), :] += row_part[row : row + 8] * col_part
        return carry

    lax.fori_loop(0, facets, add_facet, 0)

    def gather_x(d, c):
        total = blocks_ref[d, x, c]
        for k in range(1, lanes):
            x_copy(k, d, c).wait_recv()
            total = total + xrecv[k - 1, d, c]
        return total

    for t in range(levels - 1):
        d = dest(t)
        right = d > z
        way = jnp.where(right, 0, 1)
        target = jnp.where(right, z + 1, z - 1)
        fed = jnp.where(right, z > 0, z < levels - 1)
        for c in range(CHUNKS):
            zsend[d, c] = gather_x(d, c)

            @pl.when(fed)
            def _():
                z_copy(way, d, c, target).wait_recv()
                zsend[d, c] += zrecv[way, d, c]

            z_copy(way, d, c, target).start()

    for c in range(CHUNKS):
        columns = pl.ds(c * width, width)
        out_ref[:, columns] = gather_x(z, c)

        @pl.when(z > 0)
        def _():
            z_copy(0, z, c, z - 1).wait_recv()
            out_ref[:, columns] += zrecv[0, z, c]

        @pl.when(z < levels - 1)
        def _():
            z_copy(1, z, c, z + 1).wait_recv()
            out_ref[:, columns] += zrecv[1, z, c]

        stitched = out_ref[:, columns] / jnp.maximum(den[:, columns], 0.5)
        out_ref[:, columns] = stitched
        psend[:, columns] = jnp.sum(stitched * stitched, axis=0, keepdims=True)

    for k in range(1, strips):
        p_copy(k).start()
    total = psend[...]
    for k in range(1, strips):
        p_copy(k).wait_recv()
        total = total + precv[k - 1]
    power_ref[...] = total * (1.0 / (strips * height))

    for k in range(1, strips):
        p_copy(k).wait_send()
    for t in range(levels):
        d = dest(t)
        for c in range(CHUNKS):
            for k in range(1, lanes):
                x_copy(k, d, c).wait_send()
            if t < levels - 1:
                z_copy(0, d, c, jnp.where(d > z, z + 1, z - 1)).wait_send()


def body(strips, lanes, residuals, corr_rows, corr_cols, row_anchor, col_anchor, first, end, slots):
    local, fh, fw = residuals.shape
    height = fh // 4
    levels = strips // lanes
    width = fw // CHUNKS
    others = max(lanes - 1, 1)
    smem = pl.BlockSpec(memory_space=pltpu.SMEM)
    vmem = pl.BlockSpec(memory_space=pltpu.VMEM)
    dma = pltpu.SemaphoreType.DMA
    block_bytes = 4 * height * fw
    margin = 4 * 1024 * 1024
    blocks = pl.pallas_call(
        functools.partial(place_kernel, strips, lanes),
        out_shape=jax.ShapeDtypeStruct((levels, lanes, CHUNKS, height, width), jnp.float32),
        in_specs=[smem] * 5 + [vmem] * 3,
        out_specs=vmem,
        scratch_shapes=[pltpu.VMEM((local, fh + 8 + 2 * height, fw), jnp.float32)],
        compiler_params=pltpu.CompilerParams(
            vmem_limit_bytes=(strips + 11 * local) * block_bytes + margin
        ),
    )(slots, row_anchor, col_anchor, first, end, corr_rows[None, :], corr_cols[None, :], residuals)
    stitched, power = pl.pallas_call(
        functools.partial(kernel, strips, lanes),
        out_shape=(
            jax.ShapeDtypeStruct((height, fw), jnp.float32),
            jax.ShapeDtypeStruct((1, fw), jnp.float32),
        ),
        in_specs=[smem] * 4 + [vmem],
        out_specs=(vmem, vmem),
        scratch_shapes=[
            pltpu.VMEM((height, fw), jnp.float32),
            pltpu.VMEM((others, levels, CHUNKS, height, width), jnp.float32),
            pltpu.VMEM((levels, CHUNKS, height, width), jnp.float32),
            pltpu.VMEM((2, levels, CHUNKS, height, width), jnp.float32),
            pltpu.VMEM((1, fw), jnp.float32),
            pltpu.VMEM((strips - 1, 1, fw), jnp.float32),
            dma((others, levels, CHUNKS)),
            dma((others, levels, CHUNKS)),
            dma((levels, CHUNKS)),
            dma((2, levels, CHUNKS)),
            dma((strips - 1,)),
            dma((strips - 1,)),
        ],
        compiler_params=pltpu.CompilerParams(
            collective_id=0,
            has_side_effects=True,
            vmem_limit_bytes=(2 * strips + 3 * levels + 4) * block_bytes + margin,
        ),
    )(row_anchor, col_anchor, first, end, blocks)
    return stitched, power[0]


def solution(mesh):
    strips = mesh.shape["strip"]
    lanes = math.gcd(strips, max(mesh.shape["col"] // 2, 1))
    in_specs = (P("strip", None, None), P(), P(), P(), P(), P(), P(), P())
    out_specs = (P("strip", "col"), P("col"))
    run = functools.partial(body, strips, lanes)
    return jax.shard_map(run, mesh=mesh, in_specs=in_specs, out_specs=out_specs, check_vma=False)
```

```python
import functools
import math

import jax
import jax.numpy as jnp
from jax import lax
from jax.experimental import pallas as pl
from jax.experimental.pallas import tpu as pltpu
from jax.sharding import PartitionSpec as P

MESH = pl.DeviceIdType.MESH
CHUNKS = 2


def taper(position, count):
    angle = (position.astype(jnp.float32) + (0.5 - count / 2)) * (math.pi / count)
    square = angle * angle
    value = jnp.full_like(square, 1.0 / math.factorial(12))
    for order in (10, 8, 6, 4, 2, 0):
        sign = -1.0 if order % 4 == 2 else 1.0
        value = value * square + sign / math.factorial(order)
    return value * value


def visit_order(count):
    return [sorted(range(count), key=lambda d: (-abs(d - z), d < z)) for z in range(count)]


def place_kernel(
    strips, lanes, fid_hbm, ra_hbm, ca_hbm, vf_hbm, ve_hbm, rows_hbm, cols_hbm, res_hbm,
    own_ref, send_ref, fid_ref, ra_ref, ca_ref, vf_ref, ve_ref, rows_ref, cols_ref, res_ref,
    placed, sems,
):
    local, fh, fw = res_ref.shape
    height = fh // 4
    width = fw // CHUNKS
    levels = strips // lanes
    share = local // 2
    strip = lax.axis_index("strip")
    group = lax.axis_index("col")
    x = lax.rem(strip, lanes)
    core = lax.rem(group, 2)

    small = [
        (fid_hbm, fid_ref), (ra_hbm, ra_ref), (ca_hbm, ca_ref), (vf_hbm, vf_ref),
        (ve_hbm, ve_ref), (rows_hbm, rows_ref), (cols_hbm, cols_ref),
    ]
    loads = [pltpu.make_async_copy(a, b, sems.at[i]) for i, (a, b) in enumerate(small)]
    facet_loads = [
        pltpu.make_async_copy(res_hbm.at[p], res_ref.at[p], sems.at[len(small) + p])
        for p in range(local)
    ]
    for load in loads + facet_loads:
        load.start()
    blank = jnp.zeros((height, fw), jnp.float32)
    for p in range(local):
        placed[p, pl.ds(0, height), :] = blank
        placed[p, pl.ds(height + fh + 8, height), :] = blank
    y = lax.broadcasted_iota(jnp.int32, (fh, 1), 0)
    u = lax.broadcasted_iota(jnp.int32, (1, fw), 1)
    sub = lax.broadcasted_iota(jnp.int32, (8, 1), 0)
    row_taper = taper(y, fh)
    col_taper = taper(u, fw)
    eye = lax.broadcasted_iota(jnp.int32, (fh, fh), 0) == lax.broadcasted_iota(
        jnp.int32, (fh, fh), 1
    )
    for load in loads:
        load.wait()
    corr_row = jnp.sum(jnp.where(eye, rows_ref[...], 0.0), axis=1, keepdims=True)
    corr_col = jnp.concatenate([cols_ref[pl.ds(i, 1), :] for i in range(fw // 128)], axis=1)
    col_scale = col_taper * corr_col
    tiles, masks = [], []
    for p in range(local):
        f = fid_ref[strip * local + p]
        ra, ca = ra_ref[f], ca_ref[f]
        inside = (y >= vf_ref[f]) & (y < ve_ref[f])
        row_scale = jnp.where(inside, row_taper, 0.0) * corr_row
        col_pos = u + (group * fw - ca)
        masks.append((col_pos >= 0) & (col_pos < fw))
        shift = lax.rem(ca, fw)
        lift = lax.rem(ra, 8)
        tiles.append(lax.div(ra, 8))
        held = jnp.zeros((8, fw), jnp.float32)
        facet_loads[p].wait()
        for row in range(0, fh, 8):
            term = res_ref[p, pl.ds(row, 8), :] * col_scale * row_scale[row : row + 8]
            term = pltpu.roll(pltpu.roll(term, shift, axis=1), lift, axis=0)
            placed[p, pl.ds(height + row, 8), :] = jnp.where(sub < lift, held, term)
            held = term
        placed[p, pl.ds(height + fh, 8), :] = jnp.where(sub < lift, held, 0.0)

    def rows_of(p, tile, block, columns):
        start = block * (height // 8) - tile
        start = (jnp.clip(start, -height // 8, fh // 8 + 1) + height // 8) * 8
        return placed[p, pl.ds(pl.multiple_of(start, 8), height), columns]

    for c in range(CHUNKS):
        columns = pl.ds(c * width, width)
        for h in range(share):
            p = core * share + h
            tile = lax.div(ra_ref[fid_ref[strip * local + p]], 8)
            for i in range(lanes - 1):
                for k in range(4 // lanes):
                    residue = lax.rem(x + i + 1, lanes) + lanes * k
                    parts = [
                        rows_of(p, tile, residue + 4 * turn, columns)
                        for turn in range(strips // 4)
                    ]
                    send_ref[i, k, c, h] = sum(parts[1:], parts[0])
        for d in range(levels):
            total = jnp.zeros((height, width), jnp.float32)
            for p in range(local):
                part = rows_of(p, tiles[p], d * lanes + x, columns)
                total += jnp.where(masks[p][:, c * width : (c + 1) * width], part, 0.0)
            own_ref[d, c] = total


def kernel(
    strips, lanes, fid_ref, ra_ref, ca_ref, vf_ref, ve_ref, own_ref, send_ref,
    out_ref, power_ref, den, xrecv, zsend, zrecv, psend, precv,
    xs_sem, xr_sem, rs_sem, rr_sem, zs_sem, zr_sem, ps_sem, pr_sem,
):
    facets = ra_ref.shape[0]
    height, fw = out_ref.shape
    fh = 4 * height
    levels = strips // lanes
    turns = 4 // lanes
    width = fw // CHUNKS
    share = send_ref.shape[3]
    strip = lax.axis_index("strip")
    group = lax.axis_index("col")
    z, x = lax.div(strip, lanes), lax.rem(strip, lanes)
    core = lax.rem(group, 2)
    partner = group + 1 - 2 * core

    barrier = pltpu.get_barrier_semaphore()
    for k in range(1, strips):
        peer = lax.rem(strip + k, strips)
        pl.semaphore_signal(barrier, inc=1, device_id={"strip": peer}, device_id_type=MESH)
    pl.semaphore_signal(barrier, inc=1, device_id={"col": partner}, device_id_type=MESH)

    order = visit_order(levels)

    def dest(t):
        d = jnp.int32(order[0][t])
        for place_z in range(1, levels):
            d = jnp.where(z == place_z, jnp.int32(order[place_z][t]), d)
        return d

    def x_copy(i, k, c):
        return pltpu.make_async_remote_copy(
            src_ref=send_ref.at[i, k, c],
            dst_ref=xrecv.at[core, i, k, c],
            send_sem=xs_sem.at[i, k, c],
            recv_sem=xr_sem.at[i, k, c],
            device_id={"strip": z * lanes + lax.rem(x + i + 1, lanes)},
            device_id_type=MESH,
        )

    def relay(i, k, c):
        return pltpu.make_async_remote_copy(
            src_ref=xrecv.at[core, i, k, c],
            dst_ref=xrecv.at[core, i, k, c],
            send_sem=rs_sem.at[i, k, c],
            recv_sem=rr_sem.at[i, k, c],
            device_id={"col": partner},
            device_id_type=MESH,
        )

    def z_copy(way, d, c, target):
        return pltpu.make_async_remote_copy(
            src_ref=zsend.at[d, c],
            dst_ref=zrecv.at[way, d, c],
            send_sem=zs_sem.at[d, c],
            recv_sem=zr_sem.at[way, d, c],
            device_id={"strip": target * lanes + x},
            device_id_type=MESH,
        )

    def p_copy(k):
        return pltpu.make_async_remote_copy(
            src_ref=psend,
            dst_ref=precv.at[k - 1],
            send_sem=ps_sem.at[k - 1],
            recv_sem=pr_sem.at[k - 1],
            device_id={"strip": lax.rem(strip + k, strips)},
            device_id_type=MESH,
        )

    v = lax.broadcasted_iota(jnp.int32, (height, 1), 0)
    u8 = lax.broadcasted_iota(jnp.int32, (8, fw), 1) + group * fw
    den[...] = jnp.zeros_like(den)

    def add_facet(f, carry):
        row_pos = v + (strip * height - ra_ref[f])
        row_inside = (row_pos >= vf_ref[f]) & (row_pos < ve_ref[f])
        row_part = jnp.where(row_inside, taper(row_pos, fh), 0.0)
        col_pos = u8 - ca_ref[f]
        col_inside = (col_pos >= 0) & (col_pos < fw)
        col_part = jnp.where(col_inside, taper(col_pos, fw), 0.0)
        for row in range(0, height, 8):
            den[pl.ds(row, 8), :] += row_part[row : row + 8] * col_part
        return carry

    lax.fori_loop(0, facets, add_facet, 0)

    pl.semaphore_wait(barrier, strips)
    pairs = [(i, c) for c in range(CHUNKS) for i in range(lanes - 1)]
    turn = [lax.rem(dest(0) + kk, turns) for kk in range(turns)]
    for k in turn:
        for i, c in pairs:
            x_copy(i, k, c).start()

    def gather(d, c):
        total = own_ref[d, c]
        k = lax.rem(d, turns)
        u = lax.broadcasted_iota(jnp.int32, (1, width), 1) + (group * fw + c * width)
        for i in range(lanes - 1):
            source = z * lanes + lax.rem(x + lanes - i - 1, lanes)
            for p in range(2 * share):
                f = fid_ref[source * (2 * share) + p]
                row_pos = v + ((d * lanes + x) * height - ra_ref[f])
                col_pos = u - ca_ref[f]
                inside = (row_pos >= 0) & (row_pos < fh) & (col_pos >= 0) & (col_pos < fw)
                total += jnp.where(inside, xrecv[p // share, i, k, c, p % share], 0.0)
        return total

    def pass_on(k):
        for i, c in pairs:
            x_copy(i, k, c).wait_recv()
            relay(i, k, c).start()

    pass_on(turn[0])
    for i, c in pairs:
        relay(i, turn[0], c).wait_recv()
    for t in range(levels - 1):
        d = dest(t)
        right = d > z
        way = jnp.where(right, 0, 1)
        target = jnp.where(right, z + 1, z - 1)
        fed = jnp.where(right, z > 0, z < levels - 1)
        for c in range(CHUNKS):
            zsend[d, c] = gather(d, c)

            @pl.when(jnp.logical_not(fed))
            def _():
                z_copy(way, d, c, target).start()

        if t == 0:
            for k in turn[1:]:
                pass_on(k)
        for c in range(CHUNKS):

            @pl.when(fed)
            def _():
                z_copy(way, d, c, target).wait_recv()
                zsend[d, c] += zrecv[way, d, c]
                z_copy(way, d, c, target).start()

        if t == 0:
            for k in turn[1:]:
                for i, c in pairs:
                    relay(i, k, c).wait_recv()

    for c in range(CHUNKS):
        columns = pl.ds(c * width, width)
        out_ref[:, columns] = gather(z, c)
    for c in range(CHUNKS):
        columns = pl.ds(c * width, width)

        @pl.when(z > 0)
        def _():
            z_copy(0, z, c, z - 1).wait_recv()
            out_ref[:, columns] += zrecv[0, z, c]

        @pl.when(z < levels - 1)
        def _():
            z_copy(1, z, c, z + 1).wait_recv()
            out_ref[:, columns] += zrecv[1, z, c]

        stitched = out_ref[:, columns] / jnp.maximum(den[:, columns], 0.5)
        out_ref[:, columns] = stitched
        psend[:, columns] = jnp.sum(stitched * stitched, axis=0, keepdims=True)

    for k in range(1, strips):
        p_copy(k).start()
    total = psend[...]
    for k in range(1, strips):
        p_copy(k).wait_recv()
        total = total + precv[k - 1]
    total = total * (1.0 / (strips * height))
    for row in range(fw // 128):
        power_ref[pl.ds(row, 1), :] = total[:, row * 128 : (row + 1) * 128]

    for k in range(1, strips):
        p_copy(k).wait_send()
    for k in turn:
        for i, c in pairs:
            x_copy(i, k, c).wait_send()
            relay(i, k, c).wait_send()
    for t in range(levels - 1):
        d = dest(t)
        for c in range(CHUNKS):
            z_copy(0, d, c, jnp.where(d > z, z + 1, z - 1)).wait_send()


def body(strips, lanes, residuals, corr_rows, corr_cols, row_anchor, col_anchor, first, end, slots):
    local, fh, fw = residuals.shape
    height = fh // 4
    levels = strips // lanes
    turns = 4 // lanes
    share = local // 2
    width = fw // CHUNKS
    others = max(lanes - 1, 1)
    sent = (others, turns, CHUNKS, share, height, width)
    smem = pl.BlockSpec(memory_space=pltpu.SMEM)
    vmem = pl.BlockSpec(memory_space=pltpu.VMEM)
    hbm = pl.BlockSpec(memory_space=pltpu.HBM)
    dma = pltpu.SemaphoreType.DMA
    table = pltpu.SMEM(slots.shape, jnp.int32)
    block_bytes = 4 * height * fw
    margin = 4 * 1024 * 1024
    own, send = pl.pallas_call(
        functools.partial(place_kernel, strips, lanes),
        out_shape=(
            jax.ShapeDtypeStruct((levels, CHUNKS, height, width), jnp.float32),
            jax.ShapeDtypeStruct(sent, jnp.float32),
        ),
        in_specs=[hbm] * 8,
        out_specs=(vmem, vmem),
        scratch_shapes=[table] * 5
        + [
            pltpu.VMEM((1, fh), jnp.float32),
            pltpu.VMEM((fw // 128, 128), jnp.float32),
            pltpu.VMEM((local, fh, fw), jnp.float32),
            pltpu.VMEM((local, fh + 8 + 2 * height, fw), jnp.float32),
            dma((7 + local,)),
        ],
        compiler_params=pltpu.CompilerParams(
            vmem_limit_bytes=(strips + 14 * local) * block_bytes + margin
        ),
    )(
        slots, row_anchor, col_anchor, first, end,
        corr_rows[None, :], corr_cols.reshape(fw // 128, 128), residuals,
    )
    stitched, power = pl.pallas_call(
        functools.partial(kernel, strips, lanes),
        out_shape=(
            jax.ShapeDtypeStruct((height, fw), jnp.float32),
            jax.ShapeDtypeStruct((fw // 128, 128), jnp.float32),
        ),
        in_specs=[smem] * 5 + [vmem] * 2,
        out_specs=(vmem, vmem),
        scratch_shapes=[
            pltpu.VMEM((height, fw), jnp.float32),
            pltpu.VMEM((2,) + sent, jnp.float32),
            pltpu.VMEM((levels, CHUNKS, height, width), jnp.float32),
            pltpu.VMEM((2, levels, CHUNKS, height, width), jnp.float32),
            pltpu.VMEM((1, fw), jnp.float32),
            pltpu.VMEM((strips - 1, 1, fw), jnp.float32),
            dma((others, turns, CHUNKS)),
            dma((others, turns, CHUNKS)),
            dma((others, turns, CHUNKS)),
            dma((others, turns, CHUNKS)),
            dma((levels, CHUNKS)),
            dma((2, levels, CHUNKS)),
            dma((strips - 1,)),
            dma((strips - 1,)),
        ],
        compiler_params=pltpu.CompilerParams(
            collective_id=0,
            has_side_effects=True,
            vmem_limit_bytes=(2 * strips + 4 * levels + 16) * block_bytes + margin,
        ),
    )(slots, row_anchor, col_anchor, first, end, own, send)
    return stitched, power.reshape(fw)


def solution(mesh):
    strips = mesh.shape["strip"]
    lanes = math.gcd(strips, max(mesh.shape["col"] // 2, 1))
    in_specs = (P("strip", None, None), P(), P(), P(), P(), P(), P(), P())
    out_specs = (P("strip", "col"), P("col"))
    run = functools.partial(body, strips, lanes)
    return jax.shard_map(run, mesh=mesh, in_specs=in_specs, out_specs=out_specs, check_vma=False)
```

```python
import functools
import math

import jax
import jax.numpy as jnp
from jax import lax
from jax.experimental import pallas as pl
from jax.experimental.pallas import tpu as pltpu
from jax.sharding import PartitionSpec as P

MESH = pl.DeviceIdType.MESH
CHUNKS = 4
VMEM_BYTES = 67043328


def taper(position, count):
    angle = (position.astype(jnp.float32) + (0.5 - count / 2)) * (math.pi / count)
    square = angle * angle
    value = jnp.full_like(square, 1.0 / math.factorial(12))
    for order in (10, 8, 6, 4, 2, 0):
        sign = -1.0 if order % 4 == 2 else 1.0
        value = value * square + sign / math.factorial(order)
    return value * value


def visit_order(count):
    return [sorted(range(count), key=lambda d: (-abs(d - z), d < z)) for z in range(count)]


def place_kernel(
    strips, lanes, fid_hbm, ra_hbm, ca_hbm, vf_hbm, ve_hbm, rows_hbm, cols_hbm, res_hbm,
    own_ref, send_ref, fid_ref, ra_ref, ca_ref, vf_ref, ve_ref, rows_ref, cols_ref, res_ref,
    placed, sems,
):
    local, fh, fw = res_ref.shape
    height = fh // 4
    width = fw // CHUNKS
    levels = strips // lanes
    share = local // 2
    strip = lax.axis_index("strip")
    group = lax.axis_index("col")
    x = lax.rem(strip, lanes)
    core = lax.rem(group, 2)

    small = [
        (fid_hbm, fid_ref), (ra_hbm, ra_ref), (ca_hbm, ca_ref), (vf_hbm, vf_ref),
        (ve_hbm, ve_ref), (rows_hbm, rows_ref), (cols_hbm, cols_ref),
    ]
    loads = [pltpu.make_async_copy(a, b, sems.at[i]) for i, (a, b) in enumerate(small)]
    facet_loads = [
        pltpu.make_async_copy(res_hbm.at[p], res_ref.at[p], sems.at[len(small) + p])
        for p in range(local)
    ]
    for load in loads + facet_loads:
        load.start()
    blank = jnp.zeros((height, fw), jnp.float32)
    for p in range(local):
        placed[p, pl.ds(0, height), :] = blank
        placed[p, pl.ds(height + fh + 8, height), :] = blank
    y = lax.broadcasted_iota(jnp.int32, (fh, 1), 0)
    u = lax.broadcasted_iota(jnp.int32, (1, fw), 1)
    sub = lax.broadcasted_iota(jnp.int32, (8, 1), 0)
    row_taper = taper(y, fh)
    col_taper = taper(u, fw)
    eye = lax.broadcasted_iota(jnp.int32, (fh, fh), 0) == lax.broadcasted_iota(
        jnp.int32, (fh, fh), 1
    )
    for load in loads:
        load.wait()
    corr_row = jnp.sum(jnp.where(eye, rows_ref[...], 0.0), axis=1, keepdims=True)
    corr_col = jnp.concatenate([cols_ref[pl.ds(i, 1), :] for i in range(fw // 128)], axis=1)
    col_scale = col_taper * corr_col
    tiles, masks = [], []
    for p in range(local):
        f = fid_ref[strip * local + p]
        ra, ca = ra_ref[f], ca_ref[f]
        inside = (y >= vf_ref[f]) & (y < ve_ref[f])
        row_scale = jnp.where(inside, row_taper, 0.0) * corr_row
        col_pos = u + (group * fw - ca)
        masks.append((col_pos >= 0) & (col_pos < fw))
        shift = lax.rem(ca, fw)
        lift = lax.rem(ra, 8)
        tiles.append(lax.div(ra, 8))
        held = jnp.zeros((8, fw), jnp.float32)
        facet_loads[p].wait()
        for row in range(0, fh, 8):
            term = res_ref[p, pl.ds(row, 8), :] * col_scale * row_scale[row : row + 8]
            term = pltpu.roll(pltpu.roll(term, shift, axis=1), lift, axis=0)
            placed[p, pl.ds(height + row, 8), :] = jnp.where(sub < lift, held, term)
            held = term
        placed[p, pl.ds(height + fh, 8), :] = jnp.where(sub < lift, held, 0.0)

    def rows_of(p, tile, block, columns):
        start = block * (height // 8) - tile
        start = (jnp.clip(start, -height // 8, fh // 8 + 1) + height // 8) * 8
        return placed[p, pl.ds(pl.multiple_of(start, 8), height), columns]

    for c in range(CHUNKS):
        columns = pl.ds(c * width, width)
        for h in range(share):
            p = core * share + h
            tile = lax.div(ra_ref[fid_ref[strip * local + p]], 8)
            for i in range(lanes - 1):
                for k in range(4 // lanes):
                    residue = lax.rem(x + i + 1, lanes) + lanes * k
                    parts = [
                        rows_of(p, tile, residue + 4 * turn, columns)
                        for turn in range(strips // 4)
                    ]
                    send_ref[i, k, c, h] = sum(parts[1:], parts[0])
        for d in range(levels):
            total = jnp.zeros((height, width), jnp.float32)
            for p in range(local):
                part = rows_of(p, tiles[p], d * lanes + x, columns)
                total += jnp.where(masks[p][:, c * width : (c + 1) * width], part, 0.0)
            own_ref[d, c] = total


def kernel(
    strips, lanes, fid_hbm, ra_hbm, ca_hbm, vf_hbm, ve_hbm, own_hbm, send_hbm,
    out_ref, power_ref, fid_ref, ra_ref, ca_ref, vf_ref, ve_ref, own_ref, send_ref, load_sem,
    den, xrecv, zsend, zrecv, psend, precv,
    xs_sem, xr_sem, rs_sem, rr_sem, zs_sem, zr_sem, ps_sem, pr_sem,
):
    facets = ra_ref.shape[0]
    height, fw = out_ref.shape
    fh = 4 * height
    levels = strips // lanes
    turns = 4 // lanes
    width = fw // CHUNKS
    share = send_ref.shape[3]
    strip = lax.axis_index("strip")
    group = lax.axis_index("col")
    z, x = lax.div(strip, lanes), lax.rem(strip, lanes)
    core = lax.rem(group, 2)
    partner = group + 1 - 2 * core

    barrier = pltpu.get_barrier_semaphore()
    for k in range(1, strips):
        peer = lax.rem(strip + k, strips)
        pl.semaphore_signal(barrier, inc=1, device_id={"strip": peer}, device_id_type=MESH)
    pl.semaphore_signal(barrier, inc=1, device_id={"col": partner}, device_id_type=MESH)

    order = visit_order(levels)

    def dest(t):
        d = jnp.int32(order[0][t])
        for place_z in range(1, levels):
            d = jnp.where(z == place_z, jnp.int32(order[place_z][t]), d)
        return d

    def x_copy(i, k, c):
        return pltpu.make_async_remote_copy(
            src_ref=send_ref.at[i, k, c],
            dst_ref=xrecv.at[core, i, k, c],
            send_sem=xs_sem.at[i, k, c],
            recv_sem=xr_sem.at[i, k, c],
            device_id={"strip": z * lanes + lax.rem(x + i + 1, lanes)},
            device_id_type=MESH,
        )

    def relay(i, k, c):
        return pltpu.make_async_remote_copy(
            src_ref=xrecv.at[core, i, k, c],
            dst_ref=xrecv.at[core, i, k, c],
            send_sem=rs_sem.at[i, k, c],
            recv_sem=rr_sem.at[i, k, c],
            device_id={"col": partner},
            device_id_type=MESH,
        )

    def z_copy(way, d, c, target):
        return pltpu.make_async_remote_copy(
            src_ref=zsend.at[d, c],
            dst_ref=zrecv.at[way, d, c],
            send_sem=zs_sem.at[d, c],
            recv_sem=zr_sem.at[way, d, c],
            device_id={"strip": target * lanes + x},
            device_id_type=MESH,
        )

    def p_copy(k):
        return pltpu.make_async_remote_copy(
            src_ref=psend,
            dst_ref=precv.at[k - 1],
            send_sem=ps_sem.at[k - 1],
            recv_sem=pr_sem.at[k - 1],
            device_id={"strip": lax.rem(strip + k, strips)},
            device_id_type=MESH,
        )

    sources = (fid_hbm, ra_hbm, ca_hbm, vf_hbm, ve_hbm, own_hbm, send_hbm)
    targets = (fid_ref, ra_ref, ca_ref, vf_ref, ve_ref, own_ref, send_ref)
    loads = [
        pltpu.make_async_copy(a, b, load_sem.at[i])
        for i, (a, b) in enumerate(zip(sources, targets))
    ]
    for load in loads:
        load.start()

    loads[6].wait()
    pl.semaphore_wait(barrier, strips)
    pairs = [(i, c) for c in range(CHUNKS) for i in range(lanes - 1)]
    turn = [lax.rem(dest(0) + kk, turns) for kk in range(turns)]
    for k in turn:
        for i, c in pairs:
            x_copy(i, k, c).start()

    v = lax.broadcasted_iota(jnp.int32, (height, 1), 0)
    u8 = lax.broadcasted_iota(jnp.int32, (8, fw), 1) + group * fw
    for load in loads[:6]:
        load.wait()
    den[...] = jnp.zeros_like(den)

    def add_facet(f, carry):
        row_pos = v + (strip * height - ra_ref[f])
        row_inside = (row_pos >= vf_ref[f]) & (row_pos < ve_ref[f])
        row_part = jnp.where(row_inside, taper(row_pos, fh), 0.0)
        col_pos = u8 - ca_ref[f]
        col_inside = (col_pos >= 0) & (col_pos < fw)
        col_part = jnp.where(col_inside, taper(col_pos, fw), 0.0)
        for row in range(0, height, 8):
            den[pl.ds(row, 8), :] += row_part[row : row + 8] * col_part
        return carry

    lax.fori_loop(0, facets, add_facet, 0)

    def gather(d, c):
        total = own_ref[d, c]
        k = lax.rem(d, turns)
        u = lax.broadcasted_iota(jnp.int32, (1, width), 1) + (group * fw + c * width)
        for i in range(lanes - 1):
            source = z * lanes + lax.rem(x + lanes - i - 1, lanes)
            for p in range(2 * share):
                f = fid_ref[source * (2 * share) + p]
                row_pos = v + ((d * lanes + x) * height - ra_ref[f])
                col_pos = u - ca_ref[f]
                inside = (row_pos >= 0) & (row_pos < fh) & (col_pos >= 0) & (col_pos < fw)
                total += jnp.where(inside, xrecv[p // share, i, k, c, p % share], 0.0)
        return total

    def pass_on(k, c):
        for i in range(lanes - 1):
            x_copy(i, k, c).wait_recv()
            relay(i, k, c).start()

    def passed(k, c):
        for i in range(lanes - 1):
            relay(i, k, c).wait_recv()

    for t in range(levels - 1):
        d = dest(t)
        right = d > z
        way = jnp.where(right, 0, 1)
        target = jnp.where(right, z + 1, z - 1)
        fed = jnp.where(right, z > 0, z < levels - 1)
        if t == 0:
            pass_on(turn[0], 0)
        for c in range(CHUNKS):
            if t == 0:
                if c + 1 < CHUNKS:
                    pass_on(turn[0], c + 1)
                passed(turn[0], c)
            zsend[d, c] = gather(d, c)

            @pl.when(jnp.logical_not(fed))
            def _():
                z_copy(way, d, c, target).start()

        for c in range(CHUNKS):
            if t == 0:
                for k in turn[1:]:
                    pass_on(k, c)

            @pl.when(fed)
            def _():
                z_copy(way, d, c, target).wait_recv()
                zsend[d, c] += zrecv[way, d, c]
                z_copy(way, d, c, target).start()

        if t == 0:
            for k in turn[1:]:
                for c in range(CHUNKS):
                    passed(k, c)

    for c in range(CHUNKS):
        columns = pl.ds(c * width, width)
        out_ref[:, columns] = gather(z, c)
    for c in range(CHUNKS):
        columns = pl.ds(c * width, width)

        @pl.when(z > 0)
        def _():
            z_copy(0, z, c, z - 1).wait_recv()
            out_ref[:, columns] += zrecv[0, z, c]

        @pl.when(z < levels - 1)
        def _():
            z_copy(1, z, c, z + 1).wait_recv()
            out_ref[:, columns] += zrecv[1, z, c]

        stitched = out_ref[:, columns] / jnp.maximum(den[:, columns], 0.5)
        out_ref[:, columns] = stitched
        psend[:, columns] = jnp.sum(stitched * stitched, axis=0, keepdims=True)

    for k in range(1, strips):
        p_copy(k).start()
    total = psend[...]
    for k in range(1, strips):
        p_copy(k).wait_recv()
        total = total + precv[k - 1]
    total = total * (1.0 / (strips * height))
    for row in range(fw // 128):
        power_ref[pl.ds(row, 1), :] = total[:, row * 128 : (row + 1) * 128]

    for k in range(1, strips):
        p_copy(k).wait_send()
    for k in turn:
        for i, c in pairs:
            x_copy(i, k, c).wait_send()
            relay(i, k, c).wait_send()
    for t in range(levels - 1):
        d = dest(t)
        for c in range(CHUNKS):
            z_copy(0, d, c, jnp.where(d > z, z + 1, z - 1)).wait_send()


def body(strips, lanes, residuals, corr_rows, corr_cols, row_anchor, col_anchor, first, end, slots):
    local, fh, fw = residuals.shape
    height = fh // 4
    levels = strips // lanes
    turns = 4 // lanes
    share = local // 2
    width = fw // CHUNKS
    others = max(lanes - 1, 1)
    sent = (others, turns, CHUNKS, share, height, width)
    vmem = pl.BlockSpec(memory_space=pltpu.VMEM)
    hbm = pl.BlockSpec(memory_space=pltpu.HBM)
    dma = pltpu.SemaphoreType.DMA
    table = pltpu.SMEM(slots.shape, jnp.int32)
    own, send = pl.pallas_call(
        functools.partial(place_kernel, strips, lanes),
        out_shape=(
            jax.ShapeDtypeStruct((levels, CHUNKS, height, width), jnp.float32),
            jax.ShapeDtypeStruct(sent, jnp.float32),
        ),
        in_specs=[hbm] * 8,
        out_specs=(vmem, vmem),
        scratch_shapes=[table] * 5
        + [
            pltpu.VMEM((1, fh), jnp.float32),
            pltpu.VMEM((fw // 128, 128), jnp.float32),
            pltpu.VMEM((local, fh, fw), jnp.float32),
            pltpu.VMEM((local, fh + 8 + 2 * height, fw), jnp.float32),
            dma((7 + local,)),
        ],
        compiler_params=pltpu.CompilerParams(
            vmem_limit_bytes=VMEM_BYTES
        ),
    )(
        slots, row_anchor, col_anchor, first, end,
        corr_rows[None, :], corr_cols.reshape(fw // 128, 128), residuals,
    )
    stitched, power = pl.pallas_call(
        functools.partial(kernel, strips, lanes),
        out_shape=(
            jax.ShapeDtypeStruct((height, fw), jnp.float32),
            jax.ShapeDtypeStruct((fw // 128, 128), jnp.float32),
        ),
        in_specs=[hbm] * 7,
        out_specs=(vmem, vmem),
        scratch_shapes=[
            *[table] * 5,
            pltpu.VMEM((levels, CHUNKS, height, width), jnp.float32),
            pltpu.VMEM(sent, jnp.float32),
            dma((7,)),
            pltpu.VMEM((height, fw), jnp.float32),
            pltpu.VMEM((2,) + sent, jnp.float32),
            pltpu.VMEM((levels, CHUNKS, height, width), jnp.float32),
            pltpu.VMEM((2, levels, CHUNKS, height, width), jnp.float32),
            pltpu.VMEM((1, fw), jnp.float32),
            pltpu.VMEM((strips - 1, 1, fw), jnp.float32),
            dma((others, turns, CHUNKS)),
            dma((others, turns, CHUNKS)),
            dma((others, turns, CHUNKS)),
            dma((others, turns, CHUNKS)),
            dma((levels, CHUNKS)),
            dma((2, levels, CHUNKS)),
            dma((strips - 1,)),
            dma((strips - 1,)),
        ],
        compiler_params=pltpu.CompilerParams(
            collective_id=0,
            has_side_effects=True,
            vmem_limit_bytes=VMEM_BYTES,
        ),
    )(slots, row_anchor, col_anchor, first, end, own, send)
    return stitched, power.reshape(fw)


def solution(mesh):
    strips = mesh.shape["strip"]
    lanes = math.gcd(strips, max(mesh.shape["col"] // 2, 1))
    in_specs = (P("strip", None, None), P(), P(), P(), P(), P(), P(), P())
    out_specs = (P("strip", "col"), P("col"))
    run = functools.partial(body, strips, lanes)
    return jax.shard_map(run, mesh=mesh, in_specs=in_specs, out_specs=out_specs, check_vma=False)
```
